128 devices in a mesh: section: 8 (over y, core), rep: 2 (over z_hi), tp: 8 (over z_lo, x).
Axes of the slice: x: 4, y: 4, z: 4 (z_hi: 2, z_lo: 2; z = z_hi * 2 + z_lo), core: 2. Of those that a mesh axis runs over, the one named last changes fastest.
Arguments:
- token_ids: int32 [2, 8, 128], P('rep', None, 'tp'), may hold values from 0 to 16383
- embed: bfloat16 [16384, 1024], P('section'), may hold values from -6 to 6
- w_in: bfloat16 [2, 8, 2, 1024, 2816], P('rep', 'section', None, None, 'tp'), may hold values from -0.1875 to 0.1875
- w_down: bfloat16 [2, 8, 2816, 1024], P('rep', 'section', 'tp'), may hold values from -0.109375 to 0.109375
- outer_in: float32 [8, 2, 1024, 2816], P('section', None, None, 'tp'), may hold values from -0.1875 to 0.1875
- outer_down: float32 [8, 2816, 1024], P('section', 'tp'), may hold values from -0.109375 to 0.109375
- moment_in: float32 [8, 2, 1024, 2816], P('section', None, None, 'tp'), may hold values from -0.12 to 0.12
- moment_down: float32 [8, 2816, 1024], P('section', 'tp'), may hold values from -0.12 to 0.12
- cotangent: bfloat16 [2, 8, 128, 1024], P('rep', None, 'tp'), may hold values from -6 to 6
- fragment: int32 [8], replicated, may hold values 0 or 1
Outputs:
- new_in: bfloat16 [2, 8, 2, 1024, 2816], P('rep', 'section', None, None, 'tp')
- new_down: bfloat16 [2, 8, 2816, 1024], P('rep', 'section', 'tp')
- next_outer_in: float32 [8, 2, 1024, 2816], P('section', None, None, 'tp')
- next_outer_down: float32 [8, 2816, 1024], P('section', 'tp')
- next_moment_in: float32 [8, 2, 1024, 2816], P('section', None, None, 'tp')
- next_moment_down: float32 [8, 2816, 1024], P('section', 'tp')
The draws below stay inside these ranges and needn't reach their ends.
All inputs are finite; a program needn't handle non-finite values.
Results may differ from the reference program's by a relative error of at most 0.03.
Values may be sent and summed in bfloat16 or wider, within the bound.
A program may use at most 128 MiB of HBM per device.

```python
import math
import jax
import jax.numpy as jnp
import numpy as np
from jax import lax

D = 1024
FF = 2816
VOCAB = 16384
MB = 8
MTOK = 128
LAYERS_SECTION = 1
LAYERS = 8
REPS = 2
N_SECTION = 8


def place_ends(drawn, own_key, low, high):
    dims = drawn.shape
    index_at = [jax.random.randint(jax.random.fold_in(own_key, axis), (), 0, dims[axis]) for axis in range(len(dims))]
    drawn = drawn.at[tuple(index_at)].set(low)
    longest = dims.index(max(dims))
    index_at[longest] = (index_at[longest] + 1) % dims[longest]
    return drawn.at[tuple(index_at)].set(high)


def steps_of(key, shape, shards, smallest, top_value):
    def one(dim, shards_of):
        draws = jax.random.uniform(jax.random.fold_in(jax.random.fold_in(key, 6), dim), (shards_of,), jnp.float32, smallest / len(shards), top_value / len(shards))
        return jnp.repeat(jnp.exp(draws), shape[dim] // shards_of).reshape((-1,) + (1,) * (len(shape) - dim - 1))

    loudness = one(*shards[0])
    for cut in shards[1:]:
        loudness = loudness * one(*cut)
    return loudness


def rank_bounds(number_of, slope):
    loads = [(1 << 20) // math.isqrt(rank ** slope) + 1 for rank in range(1, number_of + 1)]
    scale = 1 + sum(loads) // (1 << 30)
    return np.cumsum(np.array([max(1, weight // scale) for weight in loads]))


def ranked(rng, extent, count, slope):
    listing = rank_bounds(count, slope)
    ticket = jax.random.randint(jax.random.fold_in(rng, 1), extent, 0, int(listing[count - 1]))
    grade = jnp.searchsorted(jnp.asarray(listing, jnp.int32), ticket, side="right")
    return jax.random.permutation(jax.random.fold_in(rng, 2), count)[grade].astype(jnp.int32)


def noise(key, dims, scale, most, shards=(), kind=jnp.bfloat16):
    values = scale * jax.random.normal(key, dims, jnp.float32)
    if shards:
        values = values * steps_of(key, dims, shards, -0.22, 0.18)
    return jnp.clip(values, -most, most).astype(kind)


def setup_inputs(seed: int = 0) -> dict:
    arg_keys = jax.random.split(jax.random.key(seed), 11)
    return {
        "token_ids": place_ends(ranked(arg_keys[0], (REPS, MB, MTOK), VOCAB, 2), jax.random.fold_in(arg_keys[0], 3), 0, VOCAB - 1).astype(jnp.int32),
        "embed": noise(arg_keys[1], (VOCAB, D), 1.0, 6.0, ((0, 8),)),
        "w_in": noise(arg_keys[2], (REPS, LAYERS, 2, D, FF), D ** -0.5, 0.1875, ((0, 2), (1, 8), (4, 8))),
        "w_down": noise(arg_keys[3], (REPS, LAYERS, FF, D), FF ** -0.5, 0.109375, ((0, 2), (1, 8), (2, 8))),
        "outer_in": noise(arg_keys[4], (LAYERS, 2, D, FF), D ** -0.5, 0.1875, ((0, 8), (3, 8)), jnp.float32),
        "outer_down": noise(arg_keys[5], (LAYERS, FF, D), FF ** -0.5, 0.109375, ((0, 8), (1, 8)), jnp.float32),
        "moment_in": noise(arg_keys[6], (LAYERS, 2, D, FF), 0.02, 0.12, ((0, 8), (3, 8)), jnp.float32),
        "moment_down": noise(arg_keys[7], (LAYERS, FF, D), 0.02, 0.12, ((0, 8), (1, 8)), jnp.float32),
        "cotangent": noise(arg_keys[8], (REPS, MB, MTOK, D), 1.0, 6.0, ((0, 2), (2, 8))),
        "fragment": place_ends((jax.random.randint(arg_keys[9], (N_SECTION,), 0, 2) < 1).astype(jnp.int32), jax.random.fold_in(arg_keys[9], 1), 0, 1),
    }


EPS = 1e-05
INNER_LR = 0.001
OUTER_LR = 0.7
MOMENTUM = 0.9

def scale_rows(values):
    return lax.rsqrt(lax.optimization_barrier(jnp.mean(values * values, axis=-1, keepdims=True)) + EPS)

def layer_forward(x, pair, down):
    xf = x.astype(jnp.float32)
    rinv = scale_rows(xf)
    normed = (xf * rinv).astype(jnp.bfloat16)
    gate = jnp.dot(normed, pair[0], preferred_element_type=jnp.float32)
    upper = jnp.dot(normed, pair[1], preferred_element_type=jnp.float32)
    hidden = (jax.nn.silu(gate) * upper).astype(jnp.bfloat16)
    out = jnp.dot(hidden, down, preferred_element_type=jnp.float32)
    return ((xf + out).astype(jnp.bfloat16), (normed, gate, upper, hidden))

def layer_backward(grad, x, pair, down, saved):
    normed, gate, upper, hidden = saved
    d_hidden = jnp.dot(grad, down.T, preferred_element_type=jnp.float32)
    sig = jax.nn.sigmoid(gate)
    d_gate = (d_hidden * upper * sig * (1.0 + gate * (1.0 - sig))).astype(jnp.bfloat16)
    d_upper = (d_hidden * jax.nn.silu(gate)).astype(jnp.bfloat16)
    g_down = jnp.dot(hidden.T, grad, preferred_element_type=jnp.float32)
    g_pair = jnp.stack([jnp.dot(normed.T, d_gate, preferred_element_type=jnp.float32), jnp.dot(normed.T, d_upper, preferred_element_type=jnp.float32)])
    d_norm = jnp.dot(d_gate, pair[0].T, preferred_element_type=jnp.float32) + jnp.dot(d_upper, pair[1].T, preferred_element_type=jnp.float32)
    xf = x.astype(jnp.float32)
    rinv = scale_rows(xf)
    d_x = grad.astype(jnp.float32) + rinv * d_norm - xf * (rinv * rinv * rinv) * lax.optimization_barrier(jnp.mean(d_norm * xf, axis=-1, keepdims=True))
    return (d_x.astype(jnp.bfloat16), g_pair, g_down)

def reference(token_ids, embed, w_in, w_down, outer_in, outer_down, moment_in, moment_down, cotangent, fragment):
    chosen = fragment[jnp.arange(LAYERS) // LAYERS_SECTION] == 1
    inner_in = []
    inner_down = []
    for replica in range(REPS):
        x = jnp.take(embed, token_ids[replica].reshape(-1), axis=0)
        inputs = []
        saves = []
        for layer in range(LAYERS):
            inputs.append(x)
            x, saved = layer_forward(x, w_in[replica, layer], w_down[replica, layer])
            saves.append(saved)
        grad = cotangent[replica].reshape(-1, D)
        pair_list = [None] * LAYERS
        down_list = [None] * LAYERS
        for layer in reversed(range(LAYERS)):
            grad, g_pair, g_down = layer_backward(grad, inputs[layer], w_in[replica, layer], w_down[replica, layer], saves[layer])
            pair_list[layer] = (w_in[replica, layer].astype(jnp.float32) - INNER_LR * g_pair).astype(jnp.bfloat16)
            down_list[layer] = (w_down[replica, layer].astype(jnp.float32) - INNER_LR * g_down).astype(jnp.bfloat16)
        inner_in.append(jnp.stack(pair_list))
        inner_down.append(jnp.stack(down_list))
    inner_in = jnp.stack(inner_in)
    inner_down = jnp.stack(inner_down)
    mean_in = lax.optimization_barrier(jnp.mean(outer_in[None] - inner_in.astype(jnp.float32), axis=0))
    mean_down = lax.optimization_barrier(jnp.mean(outer_down[None] - inner_down.astype(jnp.float32), axis=0))
    moment_next_in = MOMENTUM * moment_in + mean_in
    moment_next_down = MOMENTUM * moment_down + mean_down
    outer_next_in = outer_in - OUTER_LR * (mean_in + MOMENTUM * moment_next_in)
    outer_next_down = outer_down - OUTER_LR * (mean_down + MOMENTUM * moment_next_down)
    pick_in = chosen[:, None, None, None]
    pick_down = chosen[:, None, None]
    new_in = jnp.where(pick_in[None], outer_next_in.astype(jnp.bfloat16)[None], inner_in)
    new_down = jnp.where(pick_down[None], outer_next_down.astype(jnp.bfloat16)[None], inner_down)
    return (new_in, new_down, jnp.where(pick_in, outer_next_in, outer_in), jnp.where(pick_down, outer_next_down, outer_down), jnp.where(pick_in, moment_next_in, moment_in), jnp.where(pick_down, moment_next_down, moment_down))
```

```python
import functools

import jax
import jax.numpy as jnp
from jax import lax
from jax.experimental import pallas as pl
from jax.experimental.pallas import tpu as pltpu
from jax.sharding import PartitionSpec as P

EPS = 1e-05
INNER_LR = 0.001
OUTER_LR = 0.7
MOMENTUM = 0.9
MESH = pl.DeviceIdType.MESH
BF16 = jnp.bfloat16
F32 = jnp.float32
NT = (((1,), (1,)), ((), ()))
TN = (((0,), (0,)), ((), ()))


def relay_kernel(
    S, N, ZX,
    looked, cot, w_gate, w_up, w_down,
    new_gate, new_up, new_down,
    ag_f, rs_f, res_f, out_f, x_own, x_next,
    ag_b, rs_b, res_b, out_b,
    gate_s, up_s, hid_s, dg_s, du_s,
    ag_f_in, rs_f_in, res_f_in, x_next_in, ag_b_in, rs_b_in, res_b_in,
    ag_f_out, rs_f_out, res_f_out, x_next_out, ag_b_out, rs_b_out, res_b_out, emb_out,
):
    s = lax.axis_index("section")
    t = lax.axis_index("tp")
    M, _, R, D = ag_f.shape
    T = N * R
    first, final = s == 0, s == S - 1
    X = ZX
    tz, tx = t // X, lax.rem(t, X)
    hops = [(dz, dx) for dz in range(N // X) for dx in range(X) if (dz, dx) != (0, 0)]
    hops.sort(key=lambda h: -(h[0] + min(h[1], X - h[1])))
    peers = [lax.rem(tz + dz, N // X) * X + lax.rem(tx + dx, X) for dz, dx in hops]
    up_s_id = jnp.minimum(s + 1, S - 1)
    down_s_id = jnp.maximum(s - 1, 0)

    def send(src, dst, out, arrive, section, tp):
        pltpu.make_async_remote_copy(
            src_ref=src, dst_ref=dst, send_sem=out, recv_sem=arrive,
            device_id={"section": section, "tp": tp}, device_id_type=MESH,
        ).start()

    def drain(ref, sem):
        pltpu.make_async_copy(ref, ref, sem).wait()

    barrier = pltpu.get_barrier_semaphore()

    def greet(section, tp):
        pl.semaphore_signal(
            barrier, inc=1, device_id={"section": section, "tp": tp}, device_id_type=MESH
        )

    for peer in peers:
        greet(s, peer)

    @pl.when(jnp.logical_not(final))
    def _():
        for k in range(N):
            greet(up_s_id, lax.rem(t + k, N))

    @pl.when(jnp.logical_not(first))
    def _():
        for k in range(N):
            greet(down_s_id, lax.rem(t + k, N))

    @pl.when(first)
    def _():
        for other in range(2, S):
            greet(other, t)
        pl.semaphore_wait(barrier, N - 1 + N + S - 2)

    @pl.when(s == 1)
    def _():
        pl.semaphore_wait(barrier, N - 1 + 2 * N)

    @pl.when(s > 1)
    def _():
        greet(0, t)

        @pl.when(final)
        def _():
            pl.semaphore_wait(barrier, N - 1 + N + 1)

        @pl.when(jnp.logical_not(final))
        def _():
            pl.semaphore_wait(barrier, N - 1 + 2 * N + 1)

    @pl.when(jnp.logical_not(first))
    def _():
        @pl.loop(0, M)
        def _(m):
            send(looked.at[m], rs_f.at[m, s], emb_out, rs_f_in.at[m], 0, t)

    def gather_grad(m):
        for peer in peers:
            send(ag_b.at[m, t], ag_b.at[m, t], ag_b_out.at[m], ag_b_in.at[m], s, peer)

        @pl.when(jnp.logical_not(first))
        def _():
            send(ag_b.at[m, t], res_b.at[m], res_b_out.at[m], res_b_in.at[m], down_s_id, t)

    @pl.when(final)
    def _():
        @pl.loop(0, M)
        def _(m):
            ag_b[m, t] = cot[m]
            gather_grad(m)

    def rinv_of(x):
        return lax.rsqrt(jnp.mean(x * x, axis=-1, keepdims=True) + EPS)

    def forward_own(m):
        @pl.when(first)
        def _():
            drain(rs_f.at[m, pl.ds(1, S - 1)], rs_f_in.at[m])
            total = looked[m].astype(F32)
            for j in range(1, S):
                total = total + rs_f[m, j].astype(F32)
            x_own[m] = total.astype(BF16)

        @pl.when(jnp.logical_not(first))
        def _():
            drain(rs_f.at[m], rs_f_in.at[m])
            drain(res_f.at[m], res_f_in.at[m])
            total = rs_f[m, 0].astype(F32)
            for j in range(1, N):
                total = total + rs_f[m, j].astype(F32)
            x_own[m] = (res_f[m].astype(F32) + total).astype(BF16)

        x = x_own[m].astype(F32)
        ag_f[m, t] = (x * rinv_of(x)).astype(BF16)
        for peer in peers:
            send(ag_f.at[m, t], ag_f.at[m, t], ag_f_out.at[m], ag_f_in.at[m], s, peer)

        @pl.when(jnp.logical_not(final))
        def _():
            send(x_own.at[m], res_f.at[m], res_f_out.at[m], res_f_in.at[m], up_s_id, t)

        @pl.when(jnp.logical_not(first))
        def _():
            send(x_own.at[m], x_next.at[m], x_next_out.at[m], x_next_in.at[m], down_s_id, t)

    def forward_all(m):
        drain(ag_f.at[m, pl.ds(0, N - 1)], ag_f_in.at[m])
        normed = ag_f[m].reshape(T, D)
        gate = jnp.dot(normed, w_gate[...], preferred_element_type=F32)
        upper = jnp.dot(normed, w_up[...], preferred_element_type=F32)
        hidden = (jax.nn.silu(gate) * upper).astype(BF16)
        gate_s[m] = gate
        up_s[m] = upper
        hid_s[m] = hidden

        @pl.when(jnp.logical_not(final))
        def _():
            part = jnp.dot(hidden, w_down[...], preferred_element_type=F32)
            out_f[m] = part.astype(BF16).reshape(N, R, D)
            for k in range(N):
                to = lax.rem(t + k, N)
                send(out_f.at[m, to], rs_f.at[m, t], rs_f_out.at[m], rs_f_in.at[m], up_s_id, to)

    @pl.loop(0, M + 1)
    def _(step):
        @pl.when(step < M)
        def _():
            forward_own(step)

        @pl.when(step > 0)
        def _():
            forward_all(step - 1)

    def backward_own(m):
        drain(rs_b.at[m], rs_b_in.at[m])
        drain(res_b.at[m], res_b_in.at[m])
        drain(x_next.at[m], x_next_in.at[m])
        d_norm = rs_b[m, 0].astype(F32)
        for j in range(1, N):
            d_norm = d_norm + rs_b[m, j].astype(F32)
        x = x_next[m].astype(F32)
        rinv = rinv_of(x)
        d_x = (
            res_b[m].astype(F32)
            + rinv * d_norm
            - x * (rinv * rinv * rinv) * jnp.mean(d_norm * x, axis=-1, keepdims=True)
        )
        ag_b[m, t] = d_x.astype(BF16)
        gather_grad(m)

    def backward_all(m):
        drain(ag_b.at[m, pl.ds(0, N - 1)], ag_b_in.at[m])
        grad = ag_b[m].reshape(T, D)
        d_hidden = lax.dot_general(grad, w_down[...], NT, preferred_element_type=F32)
        gate = gate_s[m]
        upper = up_s[m]
        sig = jax.nn.sigmoid(gate)
        d_gate = (d_hidden * upper * sig * (1.0 + gate * (1.0 - sig))).astype(BF16)
        d_up = (d_hidden * (gate * sig)).astype(BF16)
        dg_s[m] = d_gate
        du_s[m] = d_up

        @pl.when(jnp.logical_not(first))
        def _():
            part = lax.dot_general(d_gate, w_gate[...], NT, preferred_element_type=F32)
            part = part + lax.dot_general(d_up, w_up[...], NT, preferred_element_type=F32)
            out_b[m] = part.astype(BF16).reshape(N, R, D)
            for k in range(N):
                to = lax.rem(t + k, N)
                send(out_b.at[m, to], rs_b.at[m, t], rs_b_out.at[m], rs_b_in.at[m], down_s_id, to)

    @pl.loop(0, M + 1)
    def _(step):
        @pl.when((step < M) & jnp.logical_not(final))
        def _():
            backward_own(step)

        @pl.when(step > 0)
        def _():
            backward_all(step - 1)

    H = dg_s.shape[-1]
    wide = 256

    @pl.loop(0, D // wide)
    def _(c):
        cols = pl.ds(pl.multiple_of(c * wide, wide), wide)
        normed = ag_f[:, :, :, cols].reshape(M * T, wide)
        g = lax.dot_general(normed, dg_s[...].reshape(M * T, H), TN, preferred_element_type=F32)
        new_gate[cols, :] = (w_gate[cols, :].astype(F32) - INNER_LR * g).astype(BF16)
        g = lax.dot_general(normed, du_s[...].reshape(M * T, H), TN, preferred_element_type=F32)
        new_up[cols, :] = (w_up[cols, :].astype(F32) - INNER_LR * g).astype(BF16)
        grad = ag_b[:, :, :, cols].reshape(M * T, wide)
        g = lax.dot_general(hid_s[...].reshape(M * T, H), grad, TN, preferred_element_type=F32)
        new_down[:, cols] = (w_down[:, cols].astype(F32) - INNER_LR * g).astype(BF16)

    @pl.when(jnp.logical_not(first))
    def _():
        drain(looked, emb_out)

    @pl.when(final)
    def _():
        @pl.loop(0, M)
        def _(m):
            drain(x_next.at[m], x_next_out.at[m])
            drain(out_b.at[m], rs_b_out.at[m])
            drain(res_b.at[m], res_b_out.at[m])

    @pl.when(first)
    def _():
        @pl.loop(0, M)
        def _(m):
            drain(res_f.at[m], res_f_out.at[m])
            drain(out_f.at[m], rs_f_out.at[m])

    @pl.when(jnp.logical_not(first | final))
    def _():
        @pl.loop(0, M)
        def _(m):
            drain(res_f.at[m], res_f_out.at[m])
            drain(out_f.at[m], rs_f_out.at[m])
            drain(x_next.at[m], x_next_out.at[m])
            drain(out_b.at[m], rs_b_out.at[m])
            drain(res_b.at[m], res_b_out.at[m])

    @pl.loop(0, M)
    def _(m):
        drain(ag_f.at[m, pl.ds(0, N - 1)], ag_f_out.at[m])
        drain(ag_b.at[m, pl.ds(0, N - 1)], ag_b_out.at[m])


def relay(looked, cot, pair, down):
    S, N = lax.axis_size("section"), lax.axis_size("tp")
    M, R, D = looked.shape
    H = down.shape[0]
    T = N * R
    vm = pltpu.VMEM
    dma = pltpu.SemaphoreType.DMA((M,))
    scratch = [
        vm((M, N, R, D), BF16), vm((M, N, R, D), BF16), vm((M, R, D), BF16),
        vm((M, N, R, D), BF16), vm((M, R, D), BF16), vm((M, R, D), BF16),
        vm((M, N, R, D), BF16), vm((M, N, R, D), BF16), vm((M, R, D), BF16),
        vm((M, N, R, D), BF16),
        vm((M, T, H), F32), vm((M, T, H), F32),
        vm((M, T, H), BF16), vm((M, T, H), BF16), vm((M, T, H), BF16),
    ] + [dma] * 14 + [pltpu.SemaphoreType.DMA]
    spec = pl.BlockSpec(memory_space=pltpu.VMEM)
    return pl.pallas_call(
        functools.partial(relay_kernel, S, N, 4 if N % 4 == 0 else N),
        out_shape=(
            jax.ShapeDtypeStruct((D, H), BF16),
            jax.ShapeDtypeStruct((D, H), BF16),
            jax.ShapeDtypeStruct((H, D), BF16),
        ),
        in_specs=[spec] * 5,
        out_specs=[spec] * 3,
        scratch_shapes=scratch,
        compiler_params=pltpu.CompilerParams(
            collective_id=0, has_side_effects=True, vmem_limit_bytes=56 * 1024 * 1024
        ),
        name="relay",
    )(looked, cot, pair[0], pair[1], down)


def shards(
    token_ids,
    embed,
    w_in,
    w_down,
    outer_in,
    outer_down,
    moment_in,
    moment_down,
    cotangent,
    fragment,
):
    section = lax.axis_index("section")
    replicas = lax.axis_size("rep")
    ids = token_ids[0]
    vocab_part, width = embed.shape
    local_ids = ids - section * vocab_part
    inside = (local_ids >= 0) & (local_ids < vocab_part)
    looked = jnp.take(embed, jnp.clip(local_ids, 0, vocab_part - 1), axis=0)
    looked = jnp.where(inside[:, :, None], looked, jnp.zeros_like(looked))
    pair = w_in[0, 0]
    down = w_down[0, 0]
    new_gate, new_up, new_out = relay(looked, cotangent[0], pair, down)
    new_pair = jnp.stack([new_gate, new_up])
    swap = [(r, (r + 1) % replicas) for r in range(replicas)]
    other_pair = lax.ppermute(new_pair, "rep", swap)
    other_out = lax.ppermute(new_out, "rep", swap)
    mean_pair = outer_in[0] - (new_pair.astype(F32) + other_pair.astype(F32)) / replicas
    mean_down = outer_down[0] - (new_out.astype(F32) + other_out.astype(F32)) / replicas
    flag = lax.dynamic_index_in_dim(fragment, section, 0, keepdims=False)
    chosen = flag == 1
    moment_pair = MOMENTUM * moment_in[0] + mean_pair
    moment_out = MOMENTUM * moment_down[0] + mean_down
    outer_pair = outer_in[0] - OUTER_LR * (mean_pair + MOMENTUM * moment_pair)
    outer_out = outer_down[0] - OUTER_LR * (mean_down + MOMENTUM * moment_out)
    result_pair = jnp.where(chosen, outer_pair.astype(BF16), new_pair)
    result_down = jnp.where(chosen, outer_out.astype(BF16), new_out)
    return (
        result_pair[None, None],
        result_down[None, None],
        jnp.where(chosen, outer_pair, outer_in[0])[None],
        jnp.where(chosen, outer_out, outer_down[0])[None],
        jnp.where(chosen, moment_pair, moment_in[0])[None],
        jnp.where(chosen, moment_out, moment_down[0])[None],
    )


def solution(mesh):
    return jax.shard_map(
        shards,
        mesh=mesh,
        in_specs=(
            P("rep", None, "tp"),
            P("section", None),
            P("rep", "section", None, None, "tp"),
            P("rep", "section", "tp", None),
            P("section", None, None, "tp"),
            P("section", "tp", None),
            P("section", None, None, "tp"),
            P("section", "tp", None),
            P("rep", None, "tp", None),
            P(),
        ),
        out_specs=(
            P("rep", "section", None, None, "tp"),
            P("rep", "section", "tp", None),
            P("section", None, None, "tp"),
            P("section", "tp", None),
            P("section", None, None, "tp"),
            P("section", "tp", None),
        ),
        check_vma=False,
    )
```

```python
import functools

import jax
import jax.numpy as jnp
from jax import lax
from jax.experimental import pallas as pl
from jax.experimental.pallas import tpu as pltpu
from jax.sharding import PartitionSpec as P

EPS = 1e-05
INNER_LR = 0.001
OUTER_LR = 0.7
MOMENTUM = 0.9
MESH = pl.DeviceIdType.MESH
BF16 = jnp.bfloat16
F32 = jnp.float32
NT = (((1,), (1,)), ((), ()))
TN = (((0,), (0,)), ((), ()))


def relay_kernel(
    S, N, ZX,
    looked, cot, w_in, w_down,
    new_gate, new_up, new_down,
    ag_f, rs_f, res_f, out_f, x_own, x_next,
    ag_b, rs_b, res_b, out_b,
    gate_s, up_s, hid_s, dg_s, du_s,
    ag_f_in, rs_f_in, res_f_in, x_next_in, ag_b_in, rs_b_in, res_b_in,
    ag_f_out, rs_f_out, res_f_out, x_next_out, ag_b_out, rs_b_out, res_b_out, emb_out,
):
    s = lax.axis_index("section")
    t = lax.axis_index("tp")
    M, _, R, D = ag_f.shape
    T = N * R
    first, final = s == 0, s == S - 1
    X = ZX
    tz, tx = t // X, lax.rem(t, X)
    hops = [(dz, dx) for dz in range(N // X) for dx in range(X) if (dz, dx) != (0, 0)]
    hops.sort(key=lambda h: -(h[0] + min(h[1], X - h[1])))
    peers = [lax.rem(tz + dz, N // X) * X + lax.rem(tx + dx, X) for dz, dx in hops]
    up_s_id = jnp.minimum(s + 1, S - 1)
    down_s_id = jnp.maximum(s - 1, 0)

    def send(src, dst, out, arrive, section, tp):
        pltpu.make_async_remote_copy(
            src_ref=src, dst_ref=dst, send_sem=out, recv_sem=arrive,
            device_id={"section": section, "tp": tp}, device_id_type=MESH,
        ).start()

    def drain(ref, sem):
        pltpu.make_async_copy(ref, ref, sem).wait()

    barrier = pltpu.get_barrier_semaphore()

    def greet(section, tp):
        pl.semaphore_signal(
            barrier, inc=1, device_id={"section": section, "tp": tp}, device_id_type=MESH
        )

    for peer in peers:
        greet(s, peer)

    @pl.when(jnp.logical_not(final))
    def _():
        for k in range(N):
            greet(up_s_id, lax.rem(t + k, N))

    @pl.when(jnp.logical_not(first))
    def _():
        for k in range(N):
            greet(down_s_id, lax.rem(t + k, N))

    @pl.when(first)
    def _():
        for other in range(2, S):
            greet(other, t)
        pl.semaphore_wait(barrier, N - 1 + N + S - 2)

    @pl.when(s == 1)
    def _():
        pl.semaphore_wait(barrier, N - 1 + 2 * N)

    @pl.when(s > 1)
    def _():
        greet(0, t)

        @pl.when(final)
        def _():
            pl.semaphore_wait(barrier, N - 1 + N + 1)

        @pl.when(jnp.logical_not(final))
        def _():
            pl.semaphore_wait(barrier, N - 1 + 2 * N + 1)

    @pl.when(jnp.logical_not(first))
    def _():
        @pl.loop(0, M)
        def _(m):
            send(looked.at[m], rs_f.at[m, s], emb_out, rs_f_in.at[m], 0, t)

    def gather_grad(m):
        for peer in peers:
            send(ag_b.at[m, t], ag_b.at[m, t], ag_b_out.at[m], ag_b_in.at[m], s, peer)

        @pl.when(jnp.logical_not(first))
        def _():
            send(ag_b.at[m, t], res_b.at[m], res_b_out.at[m], res_b_in.at[m], down_s_id, t)

    @pl.when(final)
    def _():
        @pl.loop(0, M)
        def _(m):
            ag_b[m, t] = cot[m]
            gather_grad(m)

    def rinv_of(x):
        return lax.rsqrt(jnp.mean(x * x, axis=-1, keepdims=True) + EPS)

    def forward_own(m):
        @pl.when(first)
        def _():
            drain(rs_f.at[m, pl.ds(1, S - 1)], rs_f_in.at[m])
            total = looked[m].astype(F32)
            for j in range(1, S):
                total = total + rs_f[m, j].astype(F32)
            x_own[m] = total.astype(BF16)

        @pl.when(jnp.logical_not(first))
        def _():
            drain(rs_f.at[m], rs_f_in.at[m])
            drain(res_f.at[m], res_f_in.at[m])
            total = rs_f[m, 0].astype(F32)
            for j in range(1, N):
                total = total + rs_f[m, j].astype(F32)
            x_own[m] = (res_f[m].astype(F32) + total).astype(BF16)

        x = x_own[m].astype(F32)
        ag_f[m, t] = (x * rinv_of(x)).astype(BF16)
        for peer in peers:
            send(ag_f.at[m, t], ag_f.at[m, t], ag_f_out.at[m], ag_f_in.at[m], s, peer)

        @pl.when(jnp.logical_not(final))
        def _():
            send(x_own.at[m], res_f.at[m], res_f_out.at[m], res_f_in.at[m], up_s_id, t)

        @pl.when(jnp.logical_not(first))
        def _():
            send(x_own.at[m], x_next.at[m], x_next_out.at[m], x_next_in.at[m], down_s_id, t)

    def forward_all(m):
        drain(ag_f.at[m, pl.ds(0, N - 1)], ag_f_in.at[m])
        normed = ag_f[m].reshape(T, D)
        gate = lax.dot_general(normed, w_in[0], NT, preferred_element_type=F32)
        upper = lax.dot_general(normed, w_in[1], NT, preferred_element_type=F32)
        hidden = (jax.nn.silu(gate) * upper).astype(BF16)
        gate_s[m] = gate
        up_s[m] = upper
        hid_s[m] = hidden

        @pl.when(jnp.logical_not(final))
        def _():
            part = jnp.dot(hidden, w_down[...], preferred_element_type=F32)
            out_f[m] = part.astype(BF16).reshape(N, R, D)
            for to in peers + [t]:
                send(out_f.at[m, to], rs_f.at[m, t], rs_f_out.at[m], rs_f_in.at[m], up_s_id, to)

    @pl.loop(0, M + 2)
    def _(step):
        own = step - jnp.where(first, 0, 1)

        @pl.when((own >= 0) & (own < M))
        def _():
            forward_own(own)

        @pl.when(step > 1)
        def _():
            forward_all(step - 2)

    def backward_own(m):
        drain(rs_b.at[m], rs_b_in.at[m])
        drain(res_b.at[m], res_b_in.at[m])
        drain(x_next.at[m], x_next_in.at[m])
        d_norm = rs_b[m, 0].astype(F32)
        for j in range(1, N):
            d_norm = d_norm + rs_b[m, j].astype(F32)
        x = x_next[m].astype(F32)
        rinv = rinv_of(x)
        d_x = (
            res_b[m].astype(F32)
            + rinv * d_norm
            - x * (rinv * rinv * rinv) * jnp.mean(d_norm * x, axis=-1, keepdims=True)
        )
        ag_b[m, t] = d_x.astype(BF16)
        gather_grad(m)

    def backward_all(m):
        drain(ag_b.at[m, pl.ds(0, N - 1)], ag_b_in.at[m])
        grad = ag_b[m].reshape(T, D)
        d_hidden = lax.dot_general(grad, w_down[...], NT, preferred_element_type=F32)
        gate = gate_s[m]
        upper = up_s[m]
        sig = jax.nn.sigmoid(gate)
        d_gate = (d_hidden * upper * sig * (1.0 + gate * (1.0 - sig))).astype(BF16)
        d_up = (d_hidden * (gate * sig)).astype(BF16)
        dg_s[m] = d_gate
        du_s[m] = d_up

        @pl.when(jnp.logical_not(first))
        def _():
            part = jnp.dot(d_gate, w_in[0], preferred_element_type=F32)
            part = part + jnp.dot(d_up, w_in[1], preferred_element_type=F32)
            out_b[m] = part.astype(BF16).reshape(N, R, D)
            for to in peers + [t]:
                send(out_b.at[m, to], rs_b.at[m, t], rs_b_out.at[m], rs_b_in.at[m], down_s_id, to)

    @pl.loop(0, M + 1)
    def _(step):
        @pl.when((step < M) & jnp.logical_not(final))
        def _():
            backward_own(step)

        @pl.when(step > 0)
        def _():
            backward_all(step - 1)

    H = dg_s.shape[-1]
    wide = 256

    @pl.loop(0, D // wide)
    def _(c):
        cols = pl.ds(pl.multiple_of(c * wide, wide), wide)
        normed = ag_f[:, :, :, cols].reshape(M * T, wide)
        g = lax.dot_general(dg_s[...].reshape(M * T, H), normed, TN, preferred_element_type=F32)
        new_gate[:, cols] = (w_in[0, :, cols].astype(F32) - INNER_LR * g).astype(BF16)
        g = lax.dot_general(du_s[...].reshape(M * T, H), normed, TN, preferred_element_type=F32)
        new_up[:, cols] = (w_in[1, :, cols].astype(F32) - INNER_LR * g).astype(BF16)
        grad = ag_b[:, :, :, cols].reshape(M * T, wide)
        g = lax.dot_general(hid_s[...].reshape(M * T, H), grad, TN, preferred_element_type=F32)
        new_down[:, cols] = (w_down[:, cols].astype(F32) - INNER_LR * g).astype(BF16)

    @pl.when(jnp.logical_not(first))
    def _():
        drain(looked, emb_out)

    @pl.when(final)
    def _():
        @pl.loop(0, M)
        def _(m):
            drain(x_next.at[m], x_next_out.at[m])
            drain(out_b.at[m], rs_b_out.at[m])
            drain(res_b.at[m], res_b_out.at[m])

    @pl.when(first)
    def _():
        @pl.loop(0, M)
        def _(m):
            drain(res_f.at[m], res_f_out.at[m])
            drain(out_f.at[m], rs_f_out.at[m])

    @pl.when(jnp.logical_not(first | final))
    def _():
        @pl.loop(0, M)
        def _(m):
            drain(res_f.at[m], res_f_out.at[m])
            drain(out_f.at[m], rs_f_out.at[m])
            drain(x_next.at[m], x_next_out.at[m])
            drain(out_b.at[m], rs_b_out.at[m])
            drain(res_b.at[m], res_b_out.at[m])

    @pl.loop(0, M)
    def _(m):
        drain(ag_f.at[m, pl.ds(0, N - 1)], ag_f_out.at[m])
        drain(ag_b.at[m, pl.ds(0, N - 1)], ag_b_out.at[m])


def relay(looked, cot, pair, down):
    S, N = lax.axis_size("section"), lax.axis_size("tp")
    M, R, D = looked.shape
    H = down.shape[0]
    T = N * R
    vm = pltpu.VMEM
    dma = pltpu.SemaphoreType.DMA((M,))
    scratch = [
        vm((M, N, R, D), BF16), vm((M, N, R, D), BF16), vm((M, R, D), BF16),
        vm((M, N, R, D), BF16), vm((M, R, D), BF16), vm((M, R, D), BF16),
        vm((M, N, R, D), BF16), vm((M, N, R, D), BF16), vm((M, R, D), BF16),
        vm((M, N, R, D), BF16),
        vm((M, T, H), F32), vm((M, T, H), F32),
        vm((M, T, H), BF16), vm((M, T, H), BF16), vm((M, T, H), BF16),
    ] + [dma] * 14 + [pltpu.SemaphoreType.DMA]
    spec = pl.BlockSpec(memory_space=pltpu.VMEM)
    return pl.pallas_call(
        functools.partial(relay_kernel, S, N, 4 if N % 4 == 0 else N),
        out_shape=(
            jax.ShapeDtypeStruct((H, D), BF16),
            jax.ShapeDtypeStruct((H, D), BF16),
            jax.ShapeDtypeStruct((H, D), BF16),
        ),
        in_specs=[spec] * 4,
        out_specs=[spec] * 3,
        scratch_shapes=scratch,
        compiler_params=pltpu.CompilerParams(
            collective_id=0, has_side_effects=True, vmem_limit_bytes=56 * 1024 * 1024
        ),
        name="relay",
    )(looked, cot, pair, down)


def outer_kernel(flag, inner, other, outer, moment, *rest):
    new, next_outer, next_moment = rest[-3:]
    chosen = flag[0] == 1
    own = inner[...].astype(F32)
    before = outer[0]
    mean = before - (own + other[...].astype(F32)) / 2
    moved = MOMENTUM * moment[0] + mean
    after = before - OUTER_LR * (mean + MOMENTUM * moved)
    new[0] = jnp.where(chosen, after, own).astype(BF16)
    next_outer[0] = jnp.where(chosen, after, before)
    next_moment[0] = jnp.where(chosen, moved, moment[0])


def outer_step(flag, inner, other, outer, moment, part, earlier=()):
    H, D = inner.shape
    rows, wide = H // 2, D // 2
    small = pl.BlockSpec((rows, wide), lambda i, j: (i, j))
    block = pl.BlockSpec((1, rows, wide), lambda i, j: (part, i, j))
    return pl.pallas_call(
        outer_kernel,
        grid=(H // rows, D // wide),
        out_shape=(
            jax.ShapeDtypeStruct(outer.shape, BF16),
            jax.ShapeDtypeStruct(outer.shape, F32),
            jax.ShapeDtypeStruct(outer.shape, F32),
        ),
        in_specs=[pl.BlockSpec(memory_space=pltpu.SMEM), small, small, block, block]
        + [pl.BlockSpec(memory_space=pl.ANY)] * len(earlier),
        out_specs=(block, block, block),
        input_output_aliases={5 + i: i for i in range(len(earlier))},
        cost_estimate=pl.CostEstimate(
            flops=10 * H * D, bytes_accessed=22 * H * D, transcendentals=0
        ),
        name="outer_step",
    )(flag, inner, other, outer, moment, *earlier)


def shards(
    token_ids,
    embed,
    w_in,
    w_down,
    outer_in,
    outer_down,
    moment_in,
    moment_down,
    cotangent,
    fragment,
):
    section = lax.axis_index("section")
    replicas = lax.axis_size("rep")
    ids = token_ids[0]
    vocab_part, width = embed.shape
    local_ids = ids - section * vocab_part
    inside = (local_ids >= 0) & (local_ids < vocab_part)
    looked = jnp.take(embed, jnp.clip(local_ids, 0, vocab_part - 1), axis=0)
    looked = jnp.where(inside[:, :, None], looked, jnp.zeros_like(looked))
    rows = 8
    looked = looked.reshape(-1, rows, width)
    seeds = cotangent.reshape(-1, rows, width)
    pair = jnp.swapaxes(w_in[0, 0], 1, 2)
    new_gate, new_up, new_out = relay(looked, seeds, pair, w_down[0, 0])
    swap = [(r, (r + 1) % replicas) for r in range(replicas)]
    flag = lax.dynamic_slice(fragment, (section,), (1,))
    outer_pair = jnp.swapaxes(outer_in[0], 1, 2)
    moment_pair = jnp.swapaxes(moment_in[0], 1, 2)
    done = outer_step(flag, new_gate, lax.ppermute(new_gate, "rep", swap), outer_pair, moment_pair, 0)
    done = outer_step(
        flag, new_up, lax.ppermute(new_up, "rep", swap), outer_pair, moment_pair, 1, done
    )
    last = outer_step(
        flag, new_out, lax.ppermute(new_out, "rep", swap), outer_down, moment_down, 0
    )
    pair_new, pair_outer, pair_moment = (jnp.swapaxes(part, 1, 2) for part in done)
    down_new, down_outer, down_moment = last
    return (
        pair_new[None, None],
        down_new[None],
        pair_outer[None],
        down_outer,
        pair_moment[None],
        down_moment,
    )


def solution(mesh):
    return jax.shard_map(
        shards,
        mesh=mesh,
        in_specs=(
            P("rep", None, "tp"),
            P("section", None),
            P("rep", "section", None, None, "tp"),
            P("rep", "section", "tp", None),
            P("section", None, None, "tp"),
            P("section", "tp", None),
            P("section", None, None, "tp"),
            P("section", "tp", None),
            P("rep", None, "tp", None),
            P(),
        ),
        out_specs=(
            P("rep", "section", None, None, "tp"),
            P("rep", "section", "tp", None),
            P("section", None, None, "tp"),
            P("section", "tp", None),
            P("section", None, None, "tp"),
            P("section", "tp", None),
        ),
        check_vma=False,
    )
```

```python
import functools

import jax
import jax.numpy as jnp
from jax import lax
from jax.experimental import pallas as pl
from jax.experimental.pallas import tpu as pltpu
from jax.sharding import PartitionSpec as P

EPS = 1e-05
INNER_LR = 0.001
OUTER_LR = 0.7
MOMENTUM = 0.9
MESH = pl.DeviceIdType.MESH
EARLY = 3
LAG = 6
BF16 = jnp.bfloat16
F32 = jnp.float32
NT = (((1,), (1,)), ((), ()))
TN = (((0,), (0,)), ((), ()))


def relay_kernel(
    S, N, ZX,
    looked, cot, w_in, w_down,
    new_gate, new_up, new_down,
    ag_f, rs_f, res_f, out_f, x_own, x_next,
    ag_b, rs_b, res_b, out_b,
    gate_s, up_s, hid_s, dg_s, du_s,
    ag_f_in, rs_f_in, res_f_in, x_next_in, ag_b_in, rs_b_in, res_b_in,
    ag_f_out, rs_f_out, res_f_out, x_next_out, ag_b_out, rs_b_out, res_b_out, emb_out, go,
):
    s = lax.axis_index("section")
    t = lax.axis_index("tp")
    M, _, R, D = ag_f.shape
    T = N * R
    first, final = s == 0, s == S - 1
    X = ZX
    tz, tx = t // X, lax.rem(t, X)
    hops = [(dz, dx) for dz in range(N // X) for dx in range(X) if (dz, dx) != (0, 0)]
    hops.sort(key=lambda h: -(h[0] + min(h[1], X - h[1])))
    peers = [lax.rem(tz + dz, N // X) * X + lax.rem(tx + dx, X) for dz, dx in hops]
    up_s_id = jnp.minimum(s + 1, S - 1)
    down_s_id = jnp.maximum(s - 1, 0)

    def send(src, dst, out, arrive, section, tp):
        pltpu.make_async_remote_copy(
            src_ref=src, dst_ref=dst, send_sem=out, recv_sem=arrive,
            device_id={"section": section, "tp": tp}, device_id_type=MESH,
        ).start()

    def drain(ref, sem):
        pltpu.make_async_copy(ref, ref, sem).wait()

    barrier = pltpu.get_barrier_semaphore()

    def greet(section, tp):
        pl.semaphore_signal(
            barrier, inc=1, device_id={"section": section, "tp": tp}, device_id_type=MESH
        )

    for peer in peers:
        greet(s, peer)

    @pl.when(jnp.logical_not(final))
    def _():
        for k in range(N):
            greet(up_s_id, lax.rem(t + k, N))

    @pl.when(jnp.logical_not(first))
    def _():
        for k in range(N):
            greet(down_s_id, lax.rem(t + k, N))

    @pl.when(first)
    def _():
        for other in range(2, S):
            greet(other, t)
        pl.semaphore_wait(barrier, N - 1 + N + S - 2)

    @pl.when(s == 1)
    def _():
        pl.semaphore_wait(barrier, N - 1 + 2 * N)

    @pl.when(s > 1)
    def _():
        greet(0, t)

        @pl.when(final)
        def _():
            pl.semaphore_wait(barrier, N - 1 + N + 1)

        @pl.when(jnp.logical_not(final))
        def _():
            pl.semaphore_wait(barrier, N - 1 + 2 * N + 1)

    @pl.when(jnp.logical_not(first))
    def _():
        @pl.loop(0, EARLY)
        def _(m):
            send(looked.at[m], rs_f.at[m, s], emb_out, rs_f_in.at[m], 0, t)

    def gather_grad(m):
        for peer in peers:
            send(ag_b.at[m, t], ag_b.at[m, t], ag_b_out.at[m], ag_b_in.at[m], s, peer)

        @pl.when(jnp.logical_not(first))
        def _():
            send(ag_b.at[m, t], res_b.at[m], res_b_out.at[m], res_b_in.at[m], down_s_id, t)

    @pl.when(final)
    def _():
        @pl.loop(0, M)
        def _(m):
            ag_b[m, t] = cot[m]
            gather_grad(m)

    def rinv_of(x):
        return lax.rsqrt(jnp.mean(x * x, axis=-1, keepdims=True) + EPS)

    def forward_own(m):
        @pl.when(first)
        def _():
            drain(rs_f.at[m, pl.ds(1, S - 1)], rs_f_in.at[m])
            total = looked[m].astype(F32)
            for j in range(1, S):
                total = total + rs_f[m, j].astype(F32)
            x_own[m] = total.astype(BF16)

        @pl.when(jnp.logical_not(first))
        def _():
            drain(rs_f.at[m], rs_f_in.at[m])
            drain(res_f.at[m], res_f_in.at[m])
            total = rs_f[m, 0].astype(F32)
            for j in range(1, N):
                total = total + rs_f[m, j].astype(F32)
            x_own[m] = (res_f[m].astype(F32) + total).astype(BF16)

        x = x_own[m].astype(F32)
        ag_f[m, t] = (x * rinv_of(x)).astype(BF16)
        for peer in peers:
            send(ag_f.at[m, t], ag_f.at[m, t], ag_f_out.at[m], ag_f_in.at[m], s, peer)

        @pl.when(jnp.logical_not(final))
        def _():
            send(x_own.at[m], res_f.at[m], res_f_out.at[m], res_f_in.at[m], up_s_id, t)

        @pl.when(jnp.logical_not(first))
        def _():
            send(x_own.at[m], x_next.at[m], x_next_out.at[m], x_next_in.at[m], down_s_id, t)

    def forward_all(m):
        drain(ag_f.at[m, pl.ds(0, N - 1)], ag_f_in.at[m])
        normed = ag_f[m].reshape(T, D)
        gate = lax.dot_general(normed, w_in[0], NT, preferred_element_type=F32)
        upper = lax.dot_general(normed, w_in[1], NT, preferred_element_type=F32)
        hidden = (jax.nn.silu(gate) * upper).astype(BF16)
        gate_s[m] = gate
        up_s[m] = upper
        hid_s[m] = hidden

        @pl.when(jnp.logical_not(final))
        def _():
            part = jnp.dot(hidden, w_down[...], preferred_element_type=F32)
            out_f[m] = part.astype(BF16).reshape(N, R, D)
            for to in peers + [t]:
                send(out_f.at[m, to], rs_f.at[m, t], rs_f_out.at[m], rs_f_in.at[m], up_s_id, to)

    def backward_own(m):
        drain(rs_b.at[m], rs_b_in.at[m])
        drain(res_b.at[m], res_b_in.at[m])
        drain(x_next.at[m], x_next_in.at[m])
        d_norm = rs_b[m, 0].astype(F32)
        for j in range(1, N):
            d_norm = d_norm + rs_b[m, j].astype(F32)
        x = x_next[m].astype(F32)
        rinv = rinv_of(x)
        d_x = (
            res_b[m].astype(F32)
            + rinv * d_norm
            - x * (rinv * rinv * rinv) * jnp.mean(d_norm * x, axis=-1, keepdims=True)
        )
        ag_b[m, t] = d_x.astype(BF16)
        gather_grad(m)

    def backward_all(m):
        drain(ag_b.at[m, pl.ds(0, N - 1)], ag_b_in.at[m])
        grad = ag_b[m].reshape(T, D)
        d_hidden = lax.dot_general(grad, w_down[...], NT, preferred_element_type=F32)
        gate = gate_s[m]
        upper = up_s[m]
        sig = jax.nn.sigmoid(gate)
        d_gate = (d_hidden * upper * sig * (1.0 + gate * (1.0 - sig))).astype(BF16)
        d_up = (d_hidden * (gate * sig)).astype(BF16)
        dg_s[m] = d_gate
        du_s[m] = d_up

        @pl.when(jnp.logical_not(first))
        def _():
            part = jnp.dot(d_gate, w_in[0], preferred_element_type=F32)
            part = part + jnp.dot(d_up, w_in[1], preferred_element_type=F32)
            out_b[m] = part.astype(BF16).reshape(N, R, D)
            for to in peers + [t]:
                send(out_b.at[m, to], rs_b.at[m, t], rs_b_out.at[m], rs_b_in.at[m], down_s_id, to)

    @pl.when(jnp.logical_not(first))
    def _():
        pl.semaphore_wait(go, 1)

        @pl.loop(EARLY, M)
        def _(m):
            send(looked.at[m], rs_f.at[m, s], emb_out, rs_f_in.at[m], 0, t)

    lag = jnp.minimum(M, LAG * (S - 1 - s))

    @pl.loop(0, M + 1 + lag)
    def _(step):
        @pl.when(step < M)
        def _():
            forward_own(step)

        @pl.when(first & (step == 0))
        def _():
            for other in range(1, S):
                pl.semaphore_signal(
                    go, inc=1, device_id={"section": other, "tp": t}, device_id_type=MESH
                )

        @pl.when((step > 0) & (step <= M))
        def _():
            forward_all(step - 1)

        back = step - lag

        @pl.when((back >= 0) & (back < M) & jnp.logical_not(final))
        def _():
            backward_own(back)

        @pl.when((back > 0) & (back <= M))
        def _():
            backward_all(back - 1)

    H = dg_s.shape[-1]
    wide = 256

    @pl.loop(0, D // wide)
    def _(c):
        cols = pl.ds(pl.multiple_of(c * wide, wide), wide)
        normed = ag_f[:, :, :, cols].reshape(M * T, wide)
        g = lax.dot_general(dg_s[...].reshape(M * T, H), normed, TN, preferred_element_type=F32)
        new_gate[:, cols] = (w_in[0, :, cols].astype(F32) - INNER_LR * g).astype(BF16)
        g = lax.dot_general(du_s[...].reshape(M * T, H), normed, TN, preferred_element_type=F32)
        new_up[:, cols] = (w_in[1, :, cols].astype(F32) - INNER_LR * g).astype(BF16)
        grad = ag_b[:, :, :, cols].reshape(M * T, wide)
        g = lax.dot_general(hid_s[...].reshape(M * T, H), grad, TN, preferred_element_type=F32)
        new_down[:, cols] = (w_down[:, cols].astype(F32) - INNER_LR * g).astype(BF16)

    @pl.when(jnp.logical_not(first))
    def _():
        drain(looked, emb_out)

    @pl.when(final)
    def _():
        @pl.loop(0, M)
        def _(m):
            drain(x_next.at[m], x_next_out.at[m])
            drain(out_b.at[m], rs_b_out.at[m])
            drain(res_b.at[m], res_b_out.at[m])

    @pl.when(first)
    def _():
        @pl.loop(0, M)
        def _(m):
            drain(res_f.at[m], res_f_out.at[m])
            drain(out_f.at[m], rs_f_out.at[m])

    @pl.when(jnp.logical_not(first | final))
    def _():
        @pl.loop(0, M)
        def _(m):
            drain(res_f.at[m], res_f_out.at[m])
            drain(out_f.at[m], rs_f_out.at[m])
            drain(x_next.at[m], x_next_out.at[m])
            drain(out_b.at[m], rs_b_out.at[m])
            drain(res_b.at[m], res_b_out.at[m])

    @pl.loop(0, M)
    def _(m):
        drain(ag_f.at[m, pl.ds(0, N - 1)], ag_f_out.at[m])
        drain(ag_b.at[m, pl.ds(0, N - 1)], ag_b_out.at[m])


def relay(looked, cot, pair, down):
    S, N = lax.axis_size("section"), lax.axis_size("tp")
    M, R, D = looked.shape
    H = down.shape[0]
    T = N * R
    vm = pltpu.VMEM
    dma = pltpu.SemaphoreType.DMA((M,))
    scratch = [
        vm((M, N, R, D), BF16), vm((M, N, R, D), BF16), vm((M, R, D), BF16),
        vm((M, N, R, D), BF16), vm((M, R, D), BF16), vm((M, R, D), BF16),
        vm((M, N, R, D), BF16), vm((M, N, R, D), BF16), vm((M, R, D), BF16),
        vm((M, N, R, D), BF16),
        vm((M, T, H), F32), vm((M, T, H), F32),
        vm((M, T, H), BF16), vm((M, T, H), BF16), vm((M, T, H), BF16),
    ] + [dma] * 14 + [pltpu.SemaphoreType.DMA, pltpu.SemaphoreType.REGULAR]
    spec = pl.BlockSpec(memory_space=pltpu.VMEM)
    return pl.pallas_call(
        functools.partial(relay_kernel, S, N, 4 if N % 4 == 0 else N),
        out_shape=(
            jax.ShapeDtypeStruct((H, D), BF16),
            jax.ShapeDtypeStruct((H, D), BF16),
            jax.ShapeDtypeStruct((H, D), BF16),
        ),
        in_specs=[spec] * 4,
        out_specs=[spec] * 3,
        scratch_shapes=scratch,
        compiler_params=pltpu.CompilerParams(
            collective_id=0, has_side_effects=True, vmem_limit_bytes=56 * 1024 * 1024
        ),
        name="relay",
    )(looked, cot, pair, down)


def outer_kernel(flag, inner, other, outer, moment, *rest):
    new, next_outer, next_moment = rest[-3:]
    chosen = flag[0] == 1
    own = inner[...].astype(F32)
    before = outer[0]
    mean = before - (own + other[...].astype(F32)) / 2
    moved = MOMENTUM * moment[0] + mean
    after = before - OUTER_LR * (mean + MOMENTUM * moved)
    new[0] = jnp.where(chosen, after, own).astype(BF16)
    next_outer[0] = jnp.where(chosen, after, before)
    next_moment[0] = jnp.where(chosen, moved, moment[0])


def outer_step(flag, inner, other, outer, moment, part, earlier=()):
    H, D = inner.shape
    rows, wide = H // 2, D // 2
    small = pl.BlockSpec((rows, wide), lambda i, j: (i, j))
    block = pl.BlockSpec((1, rows, wide), lambda i, j: (part, i, j))
    return pl.pallas_call(
        outer_kernel,
        grid=(H // rows, D // wide),
        out_shape=(
            jax.ShapeDtypeStruct(outer.shape, BF16),
            jax.ShapeDtypeStruct(outer.shape, F32),
            jax.ShapeDtypeStruct(outer.shape, F32),
        ),
        in_specs=[pl.BlockSpec(memory_space=pltpu.SMEM), small, small, block, block]
        + [pl.BlockSpec(memory_space=pl.ANY)] * len(earlier),
        out_specs=(block, block, block),
        input_output_aliases={5 + i: i for i in range(len(earlier))},
        cost_estimate=pl.CostEstimate(
            flops=10 * H * D, bytes_accessed=22 * H * D, transcendentals=0
        ),
        name="outer_step",
    )(flag, inner, other, outer, moment, *earlier)


def shards(
    token_ids,
    embed,
    w_in,
    w_down,
    outer_in,
    outer_down,
    moment_in,
    moment_down,
    cotangent,
    fragment,
):
    section = lax.axis_index("section")
    replicas = lax.axis_size("rep")
    ids = token_ids[0]
    vocab_part, width = embed.shape
    local_ids = ids - section * vocab_part
    inside = (local_ids >= 0) & (local_ids < vocab_part)
    looked = jnp.take(embed, jnp.clip(local_ids, 0, vocab_part - 1), axis=0)
    looked = jnp.where(inside[:, :, None], looked, jnp.zeros_like(looked))
    rows = 8
    looked = looked.reshape(-1, rows, width)
    seeds = cotangent.reshape(-1, rows, width)
    pair = jnp.swapaxes(w_in[0, 0], 1, 2)
    new_gate, new_up, new_out = relay(looked, seeds, pair, w_down[0, 0])
    swap = [(r, (r + 1) % replicas) for r in range(replicas)]
    flag = lax.dynamic_slice(fragment, (section,), (1,))
    outer_pair = jnp.swapaxes(outer_in[0], 1, 2)
    moment_pair = jnp.swapaxes(moment_in[0], 1, 2)
    done = outer_step(flag, new_gate, lax.ppermute(new_gate, "rep", swap), outer_pair, moment_pair, 0)
    done = outer_step(
        flag, new_up, lax.ppermute(new_up, "rep", swap), outer_pair, moment_pair, 1, done
    )
    last = outer_step(
        flag, new_out, lax.ppermute(new_out, "rep", swap), outer_down, moment_down, 0
    )
    pair_new, pair_outer, pair_moment = (jnp.swapaxes(part, 1, 2) for part in done)
    down_new, down_outer, down_moment = last
    return (
        pair_new[None, None],
        down_new[None],
        pair_outer[None],
        down_outer,
        pair_moment[None],
        down_moment,
    )


def solution(mesh):
    return jax.shard_map(
        shards,
        mesh=mesh,
        in_specs=(
            P("rep", None, "tp"),
            P("section", None),
            P("rep", "section", None, None, "tp"),
            P("rep", "section", "tp", None),
            P("section", None, None, "tp"),
            P("section", "tp", None),
            P("section", None, None, "tp"),
            P("section", "tp", None),
            P("rep", None, "tp", None),
            P(),
        ),
        out_specs=(
            P("rep", "section", None, None, "tp"),
            P("rep", "section", "tp", None),
            P("section", None, None, "tp"),
            P("section", "tp", None),
            P("section", None, None, "tp"),
            P("section", "tp", None),
        ),
        check_vma=False,
    )
```
